8 devices in a mesh: data: 1 (over z), col: 2 (over y), row: 4 (over x, core).
Axes of the slice: x: 2, y: 2, z: 1, core: 2. Of those that a mesh axis runs over, the one named last changes fastest.
Arguments:
- tokens: bfloat16 [4096, 5120], P(('data', 'row'), 'col')
- w_qkv: bfloat16 [5120, 7168], P('row', 'col')
- w_out: bfloat16 [5120, 5120], P('row', 'col')
- doc_ids: int32 [4096], P(('data', 'row'))
Outputs:
- output: bfloat16 [4096, 5120], P(('data', 'row'), 'col')
All inputs are finite; a program needn't handle non-finite values.
Results may differ from the reference program's by a relative error of at most 0.00408423.
Values are sent between devices in bfloat16 or wider.
A program may use at most 1 GiB of HBM per device.

```python
import jax
import jax.numpy as jnp
from jax import lax

HIDDEN = 5120
N_HEADS = 40
KV_HEADS = 8
HEAD_DIM = 128
SEQ_LEN = 4096
N_DOCS = 2

GROUP_RATIO = N_HEADS // KV_HEADS
QKV_COLS = HIDDEN + 2 * KV_HEADS * HEAD_DIM


def block_size(row_count, score_width):
    q_blk = row_count
    while q_blk % 16 == 0 and q_blk * score_width > 4194304:
        q_blk = q_blk // 2
    return q_blk


def setup_inputs(seed: int = 0, part: int = 0) -> dict:
    base_key = jax.random.key(seed)
    key_qkv, key_out, key_part = jax.random.split(base_key, 3)
    part_key = jax.random.fold_in(key_part, part)
    key_tok, key_doc = jax.random.split(part_key)
    tokens = jax.random.normal(key_tok, (SEQ_LEN, HIDDEN), jnp.float32).astype(jnp.bfloat16)
    w_qkv = (jax.random.normal(key_qkv, (HIDDEN, QKV_COLS), jnp.float32) * HIDDEN ** -0.5).astype(jnp.bfloat16)
    w_out = (jax.random.normal(key_out, (HIDDEN, HIDDEN), jnp.float32) * HIDDEN ** -0.5).astype(jnp.bfloat16)
    doc_cuts = jax.random.randint(key_doc, (N_DOCS - 1,), 1, SEQ_LEN, dtype=jnp.int32)
    positions = jnp.arange(SEQ_LEN, dtype=jnp.int32)
    doc_ids = jnp.sum((positions[:, None] >= doc_cuts[None, :]).astype(jnp.int32), axis=1)
    return {"tokens": tokens, "w_qkv": w_qkv, "w_out": w_out, "doc_ids": doc_ids}


def reference(tokens, w_qkv, w_out, doc_ids):
    qkv_rows = jnp.dot(tokens, w_qkv, preferred_element_type=jnp.float32).astype(jnp.bfloat16)
    qkv_rows = qkv_rows.reshape(SEQ_LEN, KV_HEADS, GROUP_RATIO + 2, HEAD_DIM)
    key_rows = qkv_rows[:, :, GROUP_RATIO, :].astype(jnp.float32)
    value_rows = qkv_rows[:, :, GROUP_RATIO + 1, :].astype(jnp.float32)
    q_blk = block_size(SEQ_LEN, N_HEADS * SEQ_LEN)
    n_steps = SEQ_LEN // q_blk
    q_steps = qkv_rows[:, :, :GROUP_RATIO, :].reshape(n_steps, q_blk, KV_HEADS, GROUP_RATIO, HEAD_DIM)
    score_scale = HEAD_DIM ** -0.5

    def attend(block_in):
        q_part, seg_part = block_in
        scores = jnp.einsum("qgrd,kgd->qgrk", q_part.astype(jnp.float32), key_rows) * score_scale
        same_doc = seg_part[:, None, None, None] == doc_ids[None, None, None, :]
        scores = jnp.where(same_doc, scores, -jnp.inf)
        weights = jax.nn.softmax(scores, axis=-1).astype(jnp.bfloat16)
        context = jnp.einsum("qgrk,kgd->qgrd", weights.astype(jnp.float32), value_rows)
        return context.astype(jnp.bfloat16)

    context = lax.map(attend, (q_steps, doc_ids.reshape(n_steps, q_blk)))
    context = context.reshape(SEQ_LEN, HIDDEN)
    return jnp.dot(context, w_out, preferred_element_type=jnp.float32).astype(jnp.bfloat16)
```

```python
import functools

import jax
import jax.numpy as jnp
from jax import lax
from jax.experimental import pallas as pl
from jax.experimental.pallas import tpu as pltpu
from jax.sharding import PartitionSpec as P

HEAD_DIM = 128
VMEM_LIMIT = 56 * 1024 * 1024
OUT_CHUNKS = (768, 768, 768, 256)


def matmul_kernel(n_own, rows, piece, x_refs, w_refs, out_ref, panel, sems):
    row = lax.axis_index("row")
    col = lax.axis_index("col")
    width = x_refs[0].shape[1]

    @pl.when(pl.program_id(0) == 0)
    def _():
        copies = []
        for i, ref in enumerate(x_refs):
            side = col if i < n_own else 1 - col
            start = (i % n_own) * width
            slot = row ^ (side * 2 + start // piece)
            if width > piece:
                for k in range(width // piece):
                    copies.append(pltpu.make_async_copy(
                        ref.at[:, pl.ds(k * piece, piece)],
                        panel.at[row ^ (side * 2 + k)], sems.at[i * 2 + k]))
            else:
                copies.append(pltpu.make_async_copy(
                    ref, panel.at[slot, :, pl.ds(start % piece, width)], sems.at[i]))
        for copy in copies:
            copy.start()
        for copy in copies:
            copy.wait()

    m_tile = 256

    @pl.loop(0, rows // m_tile)
    def _(m):
        at = pl.ds(pl.multiple_of(m * m_tile, m_tile), m_tile)
        total = jnp.dot(panel[0, at, :], w_refs[0][...], preferred_element_type=jnp.float32)
        for j in range(1, 4):
            total += jnp.dot(panel[j, at, :], w_refs[j][...], preferred_element_type=jnp.float32)
        out_ref[at, :] = total.astype(out_ref.dtype)


def panel_matmul(own, other, w_pieces):
    rows = own[0].shape[0]
    piece, cols = w_pieces[0].shape
    n_own = len(own)
    n_x = 2 * n_own
    tile = 256

    def body(*refs):
        matmul_kernel(n_own, rows, piece, refs[:n_x], refs[n_x:n_x + 4], refs[n_x + 4], refs[n_x + 5], refs[n_x + 6])

    return pl.pallas_call(
        body,
        grid=(cols // tile,),
        out_shape=jax.ShapeDtypeStruct((rows, cols), jnp.bfloat16),
        in_specs=[pl.BlockSpec(memory_space=pl.ANY)] * n_x + [pl.BlockSpec((piece, tile), lambda n: (0, n))] * 4,
        out_specs=pl.BlockSpec((rows, tile), lambda n: (0, n)),
        scratch_shapes=[pltpu.VMEM((4, rows, piece), jnp.bfloat16), pltpu.SemaphoreType.DMA((8,))],
        compiler_params=pltpu.CompilerParams(vmem_limit_bytes=VMEM_LIMIT),
        cost_estimate=pl.CostEstimate(flops=2 * rows * 4 * piece * cols, bytes_accessed=2 * 4 * piece * (rows + cols), transcendentals=0),
    )(*own, *other, *w_pieces)


def attention_kernel(n_heads, group, scale, bounds, q_ref, k0, k1, k2, k3, q_doc, k_doc, out_ref, kv_ref, sems, m_ref, l_ref, acc_ref):
    block = pl.program_id(0)
    row = lax.axis_index("row")
    q_lo, q_hi = bounds[0, block], bounds[1, block]

    @pl.when(block == 0)
    def _():
        copies = [
            pltpu.make_async_copy(ref.at[:, pl.ds(group * 2 * HEAD_DIM, 2 * HEAD_DIM)], kv_ref.at[j], sems.at[j])
            for j, ref in enumerate((k0, k1, k2, k3))
        ]
        for copy in copies:
            copy.start()
        for copy in copies:
            copy.wait()

    m_ref[...] = jnp.full_like(m_ref, -jnp.inf)
    l_ref[...] = jnp.zeros_like(l_ref)
    acc_ref[...] = jnp.zeros_like(acc_ref)

    def attend(h, j, masked):
        cols = pl.ds(pl.multiple_of(h * HEAD_DIM, HEAD_DIM), HEAD_DIM)
        scores = lax.dot_general(q_ref[:, cols], kv_ref[j, :, :HEAD_DIM], (((1,), (1,)), ((), ())), preferred_element_type=jnp.float32)
        scores = scores * scale
        if masked:
            scores = jnp.where(q_doc[...] == k_doc[row ^ j], scores, -jnp.inf)
        old = m_ref[h, :, :1]
        top = jnp.maximum(old, jnp.max(scores, axis=1, keepdims=True))
        weights = jnp.exp(scores - top)
        fade = jnp.exp(old - top)
        total = fade * l_ref[h, :, :1] + jnp.sum(weights, axis=1, keepdims=True)
        context = jnp.dot(weights.astype(jnp.bfloat16), kv_ref[j, :, HEAD_DIM:], preferred_element_type=jnp.float32)
        m_ref[h] = jnp.broadcast_to(top, m_ref.shape[1:])
        l_ref[h] = jnp.broadcast_to(total, l_ref.shape[1:])
        acc_ref[h] = fade * acc_ref[h] + context

    @pl.loop(0, 4)
    def _(j):
        k_lo, k_hi = bounds[2, row ^ j], bounds[3, row ^ j]
        same = (q_lo == q_hi) & (k_lo == k_hi) & (q_lo == k_lo)
        meets = (q_lo <= k_hi) & (k_lo <= q_hi)

        @pl.when(same)
        def _():
            @pl.loop(0, n_heads)
            def _(h):
                attend(h, j, False)

        @pl.when(meets & jnp.logical_not(same))
        def _():
            @pl.loop(0, n_heads)
            def _(h):
                attend(h, j, True)

    for h in range(n_heads):
        out_ref[:, h * HEAD_DIM:(h + 1) * HEAD_DIM] = (acc_ref[h] / l_ref[h]).astype(out_ref.dtype)


def attention(queries, group, pair_group, kv_pieces, q_doc, k_doc, bounds, n_heads, q_tile):
    rows = queries.shape[0]
    width = n_heads * HEAD_DIM
    kv_rows = kv_pieces[0].shape[0]
    grid_spec = pltpu.PrefetchScalarGridSpec(
        num_scalar_prefetch=1,
        grid=(rows // q_tile,),
        in_specs=[pl.BlockSpec((q_tile, width), lambda i, _: (i, pair_group))]
        + [pl.BlockSpec(memory_space=pl.ANY)] * 4
        + [pl.BlockSpec((q_tile, 1), lambda i, _: (i, 0)), pl.BlockSpec(k_doc.shape, lambda i, _: (0, 0, 0))],
        out_specs=pl.BlockSpec((q_tile, width), lambda i, _: (i, 0)),
        scratch_shapes=[pltpu.VMEM((4, kv_rows, 2 * HEAD_DIM), jnp.bfloat16), pltpu.SemaphoreType.DMA((4,))]
        + [pltpu.VMEM((n_heads, q_tile, HEAD_DIM), jnp.float32)] * 3,
    )
    return pl.pallas_call(
        functools.partial(attention_kernel, n_heads, group, HEAD_DIM ** -0.5),
        grid_spec=grid_spec,
        out_shape=jax.ShapeDtypeStruct((rows, width), jnp.bfloat16),
        compiler_params=pltpu.CompilerParams(vmem_limit_bytes=VMEM_LIMIT),
        cost_estimate=pl.CostEstimate(flops=4 * rows * 4 * kv_rows * width * 3, bytes_accessed=4 * rows * width, transcendentals=rows * 4 * kv_rows * n_heads),
    )(bounds, queries, *kv_pieces, q_doc, k_doc)


def solution(mesh):
    n_row = mesh.shape["row"]
    over_x = [(r, r ^ 2) for r in range(n_row)]
    over_core = [(r, r ^ 1) for r in range(n_row)]
    over_y = [(0, 1), (1, 0)]

    def spread(piece):
        far = lax.ppermute(piece, "row", over_x)
        near = lax.ppermute(piece, "row", over_core)
        return [piece, near, far, lax.ppermute(far, "row", over_core)]

    def local_block(tokens, w_qkv, w_out, doc_ids):
        rows, cols = tokens.shape
        groups = (w_qkv.shape[1] - cols) // (2 * HEAD_DIM)
        ratio = cols // HEAD_DIM // groups
        q_tile = 512

        w_parts = w_qkv.reshape(w_qkv.shape[0], groups, ratio + 2, HEAD_DIM)
        w_kv = w_parts[:, :, ratio:].reshape(w_qkv.shape[0], -1)
        w_q = [w_parts[:, g:g + 2, :ratio].reshape(w_qkv.shape[0], -1) for g in range(0, groups, 2)]

        tokens_y = lax.ppermute(tokens, "col", over_y)
        kv_w = spread(w_kv)
        q_w0 = spread(w_q[0])

        docs = lax.all_gather(doc_ids, "row", axis=0, tiled=False)
        blocks = doc_ids.reshape(rows // q_tile, q_tile)
        pad = jnp.zeros((4 - rows // q_tile,), jnp.int32)
        bounds = jnp.stack([jnp.concatenate([blocks[:, 0], pad]), jnp.concatenate([blocks[:, -1], pad]), docs[:, 0], docs[:, -1]])
        q_doc = doc_ids.reshape(rows, 1)
        k_doc = docs.reshape(n_row, 1, rows)

        kv = panel_matmul([tokens], [tokens_y], kv_w)
        kv_pieces = spread(kv)
        w_q1, _ = lax.optimization_barrier((w_q[1], kv))
        q_w1 = spread(w_q1)
        edges = [0]
        for width in OUT_CHUNKS:
            edges.append(edges[-1] + width)
        out_w = [spread(w_out[:, lo:hi]) for lo, hi in zip(edges, edges[1:])]

        own, other = [], []
        for pair, weights in enumerate((q_w0, q_w1)):
            queries = panel_matmul([tokens], [tokens_y], weights)
            for g in range(2):
                context = attention(queries, 2 * pair + g, g, kv_pieces, q_doc, k_doc, bounds, ratio, q_tile)
                own.append(context)
                other.append(lax.ppermute(context, "col", over_y))
        parts = [panel_matmul(own, other, weights) for weights in out_w]
        return jnp.concatenate(parts, axis=1)

    row_spec = P(("data", "row"), "col")
    weight_spec = P("row", "col")
    return jax.shard_map(local_block, mesh=mesh, in_specs=(row_spec, weight_spec, weight_spec, P(("data", "row"))), out_specs=row_spec, check_vma=False)
```

```python
import functools

import jax
import jax.numpy as jnp
from jax import lax
from jax.experimental import pallas as pl
from jax.experimental.pallas import tpu as pltpu
from jax.sharding import PartitionSpec as P


HEAD_DIM = 128
LOG2E = 1.4426950408889634
VMEM_LIMIT = 60 * 1024 * 1024
OUT_CHUNKS = 4
Q_TILE = 512


def n_tiles(width):
    return [(lo, min(256, width - lo)) for lo in range(0, width, 256)]


def project_kernel(n_own, piece, offset, width, splits, refs):
    xs, (w_own, w_near, w_far, w_last) = refs[:2 * n_own], refs[2 * n_own:2 * n_own + 4]
    outs = refs[-5 - len(splits):-5]
    panel, weights, total, x_sems, w_sems = refs[-5:]
    row, col = lax.axis_index("row"), lax.axis_index("col")
    x_width = 2 * piece // n_own
    parts = max(piece // x_width, 1)
    copies = []
    for i, ref in enumerate(xs):
        side = col if i < n_own else 1 - col
        start = (i % n_own) * x_width
        for lo in range(0, x_width, min(x_width, piece)):
            at = start + lo
            slot = row ^ (side * 2 + at // piece)
            size = min(x_width, piece)
            copies.append(pltpu.make_async_copy(
                ref.at[:, pl.ds(lo, size)], panel.at[slot, :, pl.ds(at % piece, size)],
                x_sems.at[slot, (at % piece) // size]))
    columns = pl.ds(offset, width)
    w_copies = [
        pltpu.make_async_copy(w_own.at[:, columns], weights.at[0], w_sems.at[0]),
        pltpu.make_async_copy(w_near.at[:, columns], weights.at[1], w_sems.at[1]),
        pltpu.make_async_copy(w_far, weights.at[2], w_sems.at[2]),
        pltpu.make_async_copy(w_last, weights.at[3], w_sems.at[3]),
    ]
    w_copies[0].start()
    for copy in copies:
        copy.start()
    for copy in w_copies[1:]:
        copy.start()
    size = min(x_width, piece)
    for j in range(4):
        w_copies[j].wait()
        for k in range(parts):
            at = panel.at[j, :, pl.ds(k * size, size)]
            pltpu.make_async_copy(at, at, x_sems.at[j, k]).wait()
        for lo, n in n_tiles(width):
            here = pl.ds(lo, n)
            term = jnp.dot(panel[j], weights[j, :, here], preferred_element_type=jnp.float32)
            if j > 0:
                term += total[:, here]
            if j < 3:
                total[:, here] = term
            else:
                for out, first, last in zip(outs, (0,) + splits[:-1], splits):
                    a, b = max(lo, first), min(lo + n, last)
                    if a < b:
                        out[:, a - first:b - first] = term[:, a - lo:b - lo].astype(out.dtype)


def project(own, other, w_own, w_near, w_far, w_last, offset, splits):
    rows = own[0].shape[0]
    piece, width = w_far.shape
    n_own = len(own)
    ends = (0,) + splits[:-1]

    def body(*refs):
        project_kernel(n_own, piece, offset, width, splits, refs)

    return pl.pallas_call(
        body,
        out_shape=[jax.ShapeDtypeStruct((rows, b - a), jnp.bfloat16) for a, b in zip(ends, splits)],
        in_specs=[pl.BlockSpec(memory_space=pl.ANY)] * (2 * n_own + 4),
        out_specs=[pl.BlockSpec(memory_space=pltpu.VMEM)] * len(splits),
        scratch_shapes=[
            pltpu.VMEM((4, rows, piece), jnp.bfloat16),
            pltpu.VMEM((4, piece, width), jnp.bfloat16),
            pltpu.VMEM((rows, width), jnp.float32),
            pltpu.SemaphoreType.DMA((4, 2)),
            pltpu.SemaphoreType.DMA((4,)),
        ],
        compiler_params=pltpu.CompilerParams(vmem_limit_bytes=VMEM_LIMIT),
        cost_estimate=pl.CostEstimate(flops=2 * rows * 4 * piece * width, bytes_accessed=8 * piece * (rows + width), transcendentals=0),
    )(*own, *other, w_own, w_near, w_far, w_last)


def attention_kernel(n, bq, docs, q_ref, k0, k1, k2, k3, q_doc, k_doc, out_ref, kv, sems, p0, p1, l0, l1, acc, big):
    i = pl.program_id(0)
    row = lax.axis_index("row")
    bk = k0.shape[0]
    d = HEAD_DIM

    @pl.when(i == 0)
    def _():
        copies = [pltpu.make_async_copy(ref, kv.at[row ^ j], sems.at[j]) for j, ref in enumerate((k0, k1, k2, k3))]
        for copy in copies:
            copy.start()
        for copy in copies:
            copy.wait()

    def ends(kb):
        at = (row ^ kb) * bk
        return docs[at], docs[at + bk - 1]

    q_lo, q_hi = docs[i * bq], docs[i * bq + bq - 1]
    lo, hi = jnp.int32(0), jnp.int32(0)
    for kb in range(4):
        k_lo, k_hi = ends(kb)
        lo += (k_hi < q_lo).astype(jnp.int32)
        hi += (k_lo <= q_hi).astype(jnp.int32)

    scale = d ** -0.5 * LOG2E
    probs, sums = (p0, p1), (l0, l1)

    def cols_of(u):
        return pl.ds(pl.multiple_of(u * d, d), d)

    def fold(x, op):
        y = x[:, :d]
        for t in range(1, bk // d):
            y = op(y, x[:, t * d:(t + 1) * d])
        return y

    def scores(u, kb, masked):
        s = lax.dot_general(q_ref[:, cols_of(u)], kv[kb, :, :d], (((1,), (1,)), ((), ())), preferred_element_type=jnp.float32)
        if masked:
            s = jnp.where(q_doc[...] == k_doc[row ^ kb], s, -jnp.inf)
        return s

    def stage(first, second, phase, exact=False):
        p_a, l_a = probs[phase % 2], sums[phase % 2]
        p_c, l_c = probs[(phase - 1) % 2], sums[(phase - 1) % 2]
        if first is not None:
            if exact:
                acc[...] = jnp.full(acc.shape, -jnp.inf, jnp.float32)

                @pl.loop(lo, hi)
                def _(kb):
                    acc[...] = jnp.maximum(acc[...], fold(scores(first, kb, True), jnp.maximum))

                top = jnp.max(acc[...], axis=1, keepdims=True)
            else:
                own = kv[row, pl.ds(pl.multiple_of(i * bq, bq), bq), :d].astype(jnp.float32)
                top = jnp.sum(q_ref[:, cols_of(first)].astype(jnp.float32) * own, axis=1, keepdims=True)
            l_a[...] = jnp.zeros_like(l_a)
        if second is not None:
            total = jnp.sum(l_c[...], axis=1, keepdims=True)
            if not exact:
                big[...] = jnp.maximum(big[...], total)
            inv = 1.0 / total
            acc[...] = jnp.zeros_like(acc)

        def step(kb, masked):
            if second is not None:
                p = (p_c[kb] * inv).astype(jnp.bfloat16)
                acc[...] += jnp.dot(p, kv[kb, :, d:], preferred_element_type=jnp.float32)
            if first is not None:
                p = jnp.exp2((scores(first, kb, masked) - top) * scale)
                p_a[kb] = p
                l_a[...] += fold(p, jnp.add)

        @pl.loop(lo, hi)
        def _(kb):
            if first is None or exact:
                step(kb, exact)
            else:
                k_lo, k_hi = ends(kb)
                plain = (q_lo == q_hi) & (q_lo == k_lo) & (q_lo == k_hi)

                @pl.when(plain)
                def _():
                    step(kb, False)

                @pl.when(jnp.logical_not(plain))
                def _():
                    step(kb, True)

        if second is not None:
            out_ref[:, cols_of(second)] = acc[...].astype(out_ref.dtype)

    big[...] = jnp.zeros_like(big)
    stage(0, None, 0)

    @pl.loop(0, (n - 1) // 2)
    def _(k):
        stage(2 * k + 1, 2 * k, 1)
        stage(2 * k + 2, 2 * k + 1, 2)

    for u in range(1 + 2 * ((n - 1) // 2), n):
        stage(u, u - 1, u)
    stage(None, n - 1, n)

    @pl.when(jnp.logical_not(jnp.max(big[...]) < 1e30))
    def _():
        @pl.loop(0, n)
        def _(u):
            stage(u, None, 0, True)
            stage(None, u, 1, True)


def attention(queries, kv_pieces, docs, q_doc, k_doc):
    rows, width = queries.shape
    n = width // HEAD_DIM
    bk = kv_pieces[0].shape[0]
    bq = min(Q_TILE, rows)
    grid_spec = pltpu.PrefetchScalarGridSpec(
        num_scalar_prefetch=1,
        grid=(rows // bq,),
        in_specs=[pl.BlockSpec((bq, width), lambda i, _: (i, 0))]
        + [pl.BlockSpec(memory_space=pl.ANY)] * 4
        + [pl.BlockSpec((bq, 1), lambda i, _: (i, 0)), pl.BlockSpec(k_doc.shape, lambda i, _: (0, 0, 0))],
        out_specs=pl.BlockSpec((bq, width), lambda i, _: (i, 0)),
        scratch_shapes=[pltpu.VMEM((4, bk, 2 * HEAD_DIM), jnp.bfloat16), pltpu.SemaphoreType.DMA((4,))]
        + [pltpu.VMEM((4, bq, bk), jnp.float32)] * 2
        + [pltpu.VMEM((bq, HEAD_DIM), jnp.float32)] * 3
        + [pltpu.VMEM((bq, 1), jnp.float32)],
    )
    return pl.pallas_call(
        functools.partial(attention_kernel, n, bq),
        grid_spec=grid_spec,
        out_shape=jax.ShapeDtypeStruct((rows, width), jnp.bfloat16),
        compiler_params=pltpu.CompilerParams(vmem_limit_bytes=VMEM_LIMIT),
        cost_estimate=pl.CostEstimate(flops=16 * rows * 4 * bk * width, bytes_accessed=4 * rows * width, transcendentals=rows * 4 * bk * n),
    )(docs, queries, *kv_pieces, q_doc, k_doc)


def solution(mesh):
    n_row = mesh.shape["row"]
    over_x = [(r, r ^ 2) for r in range(n_row)]
    over_core = [(r, r ^ 1) for r in range(n_row)]
    over_y = [(0, 1), (1, 0)]

    def far(piece):
        return lax.ppermute(piece, "row", over_x)

    def near(piece):
        return lax.ppermute(piece, "row", over_core)

    def after(value, *others):
        return lax.optimization_barrier((value,) + others)[0]

    def local_block(tokens, w_qkv, w_out, doc_ids):
        rows, cols = tokens.shape
        groups = (w_qkv.shape[1] - cols) // (2 * HEAD_DIM)
        q_cols = cols // groups
        g_cols = q_cols + 2 * HEAD_DIM
        n_cols = cols // OUT_CHUNKS

        tokens_y = lax.ppermute(tokens, "col", over_y)
        docs_x = far(doc_ids)
        w_far = [far(w_qkv[:, g * g_cols:(g + 1) * g_cols]) for g in range(3)]
        w_near = near(w_qkv)
        docs = jnp.concatenate([doc_ids, near(doc_ids), docs_x, near(docs_x)])
        q_doc, k_doc = doc_ids.reshape(rows, 1), docs.reshape(n_row, 1, rows)
        wo_near = near(w_out)
        wo_far = []

        def project_group(g, x_y):
            w_last = near(w_far[g])
            q, kv = project([tokens], [x_y], w_qkv, w_near, w_far[g], w_last, g * g_cols, (q_cols, g_cols))
            kv_x = far(kv)
            return q, [kv, near(kv), kv_x, near(kv_x)]

        own, other = [], []

        def attend(q, pieces):
            context = attention(q, pieces, docs, q_doc, k_doc)
            own.append(context)
            other.append(lax.ppermute(context, "col", over_y))

        q0, kv0 = project_group(0, tokens_y)
        q1, kv1 = project_group(1, after(tokens_y, kv0[0]))
        q2, kv2 = project_group(2, after(tokens_y, kv1[0]))
        w_far.append(far(after(w_qkv[:, 3 * g_cols:], kv2[0])))
        wo_far.append(far(after(w_out[:, :n_cols], kv2[0])))
        attend(after(q0, q2), kv0)
        attend(after(q1, own[0]), kv1)
        q3, kv3 = project_group(3, after(tokens_y, own[1]))
        for c in range(1, OUT_CHUNKS):
            wo_far.append(far(after(w_out[:, c * n_cols:(c + 1) * n_cols], kv3[0])))
        attend(after(q2, kv3[0]), kv2)
        attend(after(q3, own[2]), kv3)
        parts = [
            project(own, other, w_out, wo_near, wo_far[c], near(wo_far[c]), c * n_cols, (n_cols,))[0]
            for c in range(OUT_CHUNKS)
        ]
        return jnp.concatenate(parts, axis=1)

    row_spec = P(("data", "row"), "col")
    weight_spec = P("row", "col")
    return jax.shard_map(local_block, mesh=mesh, in_specs=(row_spec, weight_spec, weight_spec, P(("data", "row"))), out_specs=row_spec, check_vma=False)
```

```python
import functools

import jax
import jax.numpy as jnp
from jax import lax
from jax.experimental import pallas as pl
from jax.experimental.pallas import tpu as pltpu
from jax.sharding import PartitionSpec as P


HEAD_DIM = 128
LOG2E = 1.4426950408889634
VMEM_LIMIT = 60 * 1024 * 1024
OUT_CHUNKS = (512, 1280, 768)
Q_TILE = 512


def n_tiles(width):
    return [(lo, min(256, width - lo)) for lo in range(0, width, 256)]


def project_kernel(n_own, piece, offset, width, splits, refs):
    xs, (w_own, w_near, w_far, w_last) = refs[:2 * n_own], refs[2 * n_own:2 * n_own + 4]
    outs = refs[-5 - len(splits):-5]
    panel, weights, total, x_sems, w_sems = refs[-5:]
    row, col = lax.axis_index("row"), lax.axis_index("col")
    x_width = 2 * piece // n_own
    parts = max(piece // x_width, 1)
    copies = []
    for i, ref in enumerate(xs):
        side = col if i < n_own else 1 - col
        start = (i % n_own) * x_width
        for lo in range(0, x_width, min(x_width, piece)):
            at = start + lo
            slot = row ^ (side * 2 + at // piece)
            size = min(x_width, piece)
            copies.append(pltpu.make_async_copy(
                ref.at[:, pl.ds(lo, size)], panel.at[slot, :, pl.ds(at % piece, size)],
                x_sems.at[slot, (at % piece) // size]))
    columns = pl.ds(offset, width)
    w_copies = [
        pltpu.make_async_copy(w_own.at[:, columns], weights.at[0], w_sems.at[0]),
        pltpu.make_async_copy(w_near.at[:, columns], weights.at[1], w_sems.at[1]),
        pltpu.make_async_copy(w_far, weights.at[2], w_sems.at[2]),
        pltpu.make_async_copy(w_last, weights.at[3], w_sems.at[3]),
    ]
    w_copies[0].start()
    for copy in copies:
        copy.start()
    for copy in w_copies[1:]:
        copy.start()
    size = min(x_width, piece)
    for j in range(4):
        w_copies[j].wait()
        for k in range(parts):
            at = panel.at[j, :, pl.ds(k * size, size)]
            pltpu.make_async_copy(at, at, x_sems.at[j, k]).wait()
        for lo, n in n_tiles(width):
            here = pl.ds(lo, n)
            term = jnp.dot(panel[j], weights[j, :, here], preferred_element_type=jnp.float32)
            if j > 0:
                term += total[:, here]
            if j < 3:
                total[:, here] = term
            else:
                for out, first, last in zip(outs, (0,) + splits[:-1], splits):
                    a, b = max(lo, first), min(lo + n, last)
                    if a < b:
                        out[:, a - first:b - first] = term[:, a - lo:b - lo].astype(out.dtype)


def project(own, other, w_own, w_near, w_far, w_last, offset, splits):
    rows = own[0].shape[0]
    piece, width = w_far.shape
    n_own = len(own)
    ends = (0,) + splits[:-1]

    def body(*refs):
        project_kernel(n_own, piece, offset, width, splits, refs)

    return pl.pallas_call(
        body,
        out_shape=[jax.ShapeDtypeStruct((rows, b - a), jnp.bfloat16) for a, b in zip(ends, splits)],
        in_specs=[pl.BlockSpec(memory_space=pl.ANY)] * (2 * n_own + 4),
        out_specs=[pl.BlockSpec(memory_space=pltpu.VMEM)] * len(splits),
        scratch_shapes=[
            pltpu.VMEM((4, rows, piece), jnp.bfloat16),
            pltpu.VMEM((4, piece, width), jnp.bfloat16),
            pltpu.VMEM((rows, width), jnp.float32),
            pltpu.SemaphoreType.DMA((4, 2)),
            pltpu.SemaphoreType.DMA((4,)),
        ],
        compiler_params=pltpu.CompilerParams(vmem_limit_bytes=VMEM_LIMIT),
        cost_estimate=pl.CostEstimate(flops=2 * rows * 4 * piece * width, bytes_accessed=8 * piece * (rows + width), transcendentals=0),
    )(*own, *other, w_own, w_near, w_far, w_last)


def combine_kernel(spots, piece, refs):
    n_x = len(spots)
    xs, ws, out = refs[:n_x], refs[n_x:n_x + 4], refs[-3]
    panel, sems = refs[-2:]
    row, col = lax.axis_index("row"), lax.axis_index("col")

    def copy_of(i):
        is_own, at, top = spots[i]
        side = col if is_own else 1 - col
        height, width = xs[i].shape
        return pltpu.make_async_copy(
            xs[i], panel.at[row ^ (side * 2 + at // piece), pl.ds(top, height), pl.ds(at % piece, width)], sems.at[i])

    @pl.when(pl.program_id(0) == 0)
    def _():
        for i in range(n_x):
            copy_of(i).start()
        for i in range(n_x):
            copy_of(i).wait()

    total = jnp.dot(panel[0], ws[0][...], preferred_element_type=jnp.float32)
    for j in range(1, 4):
        total += jnp.dot(panel[j], ws[j][...], preferred_element_type=jnp.float32)
    out[...] = total.astype(out.dtype)


def combine(xs, spots, rows, w_own, w_near, w_far, w_last, first, base):
    piece, width = w_far.shape
    tile = 256
    skip = first // tile
    whole = pl.BlockSpec((piece, tile), lambda n: (0, n + skip))
    chunk = pl.BlockSpec((piece, tile), lambda n: (0, n))
    extra = [] if base is None else [base]

    def body(*refs):
        kept = refs[:len(xs) + 4] + refs[len(xs) + 4 + len(extra):]
        combine_kernel(spots, piece, kept)

    return pl.pallas_call(
        body,
        grid=(width // tile,),
        out_shape=jax.ShapeDtypeStruct((rows, w_own.shape[1]), jnp.bfloat16),
        in_specs=[pl.BlockSpec(memory_space=pl.ANY)] * len(xs) + [whole, whole, chunk, chunk]
        + [pl.BlockSpec(memory_space=pl.ANY)] * len(extra),
        out_specs=pl.BlockSpec((rows, tile), lambda n: (0, n + skip)),
        scratch_shapes=[pltpu.VMEM((4, rows, piece), jnp.bfloat16), pltpu.SemaphoreType.DMA((len(xs),))],
        input_output_aliases={len(xs) + 4: 0} if extra else {},
        compiler_params=pltpu.CompilerParams(vmem_limit_bytes=VMEM_LIMIT),
        cost_estimate=pl.CostEstimate(flops=2 * rows * 4 * piece * width, bytes_accessed=8 * piece * (rows + width), transcendentals=0),
    )(*xs, w_own, w_near, w_far, w_last, *extra)


def attention_kernel(heads, bq, start, docs, q_ref, k0, k1, k2, k3, q_doc, k_doc, out_ref, kv, sems, p0, p1, l0, l1, acc, big):
    rows = q_ref.shape[0]
    n = heads * (rows // bq)
    row = lax.axis_index("row")
    bk = k0.shape[0]
    d = HEAD_DIM

    copies = [pltpu.make_async_copy(ref, kv.at[row ^ j], sems.at[j]) for j, ref in enumerate((k0, k1, k2, k3))]
    for copy in copies:
        copy.start()
    for copy in copies:
        copy.wait()

    def ends(kb):
        at = (row ^ kb) * bk
        return docs[at], docs[at + bk - 1]

    q_lo, q_hi = docs[start], docs[start + rows - 1]
    lo, hi = jnp.int32(0), jnp.int32(0)
    for kb in range(4):
        k_lo, k_hi = ends(kb)
        lo += (k_hi < q_lo).astype(jnp.int32)
        hi += (k_lo <= q_hi).astype(jnp.int32)

    scale = d ** -0.5 * LOG2E
    probs, sums = (p0, p1), (l0, l1)

    def cols_of(u):
        return pl.ds(pl.multiple_of(u % heads * d, d), d)

    def rows_of(u):
        return pl.ds(pl.multiple_of(u // heads * bq, bq), bq)

    def fold(x, op):
        y = x[:, :d]
        for t in range(1, bk // d):
            y = op(y, x[:, t * d:(t + 1) * d])
        return y

    def scores(u, kb, masked):
        s = lax.dot_general(q_ref[rows_of(u), cols_of(u)], kv[kb, :, :d], (((1,), (1,)), ((), ())), preferred_element_type=jnp.float32)
        if masked:
            s = jnp.where(q_doc[rows_of(u), :] == k_doc[row ^ kb], s, -jnp.inf)
        return s

    def stage(first, second, phase, exact=False):
        p_a, l_a = probs[phase % 2], sums[phase % 2]
        p_c, l_c = probs[(phase - 1) % 2], sums[(phase - 1) % 2]
        if first is not None:
            if exact:
                acc[...] = jnp.full(acc.shape, -jnp.inf, jnp.float32)

                @pl.loop(lo, hi)
                def _(kb):
                    acc[...] = jnp.maximum(acc[...], fold(scores(first, kb, True), jnp.maximum))

                top = jnp.max(acc[...], axis=1, keepdims=True)
            else:
                own = kv[row, pl.ds(pl.multiple_of(start + first // heads * bq, bq), bq), :d].astype(jnp.float32)
                top = jnp.sum(q_ref[rows_of(first), cols_of(first)].astype(jnp.float32) * own, axis=1, keepdims=True)
            l_a[...] = jnp.zeros_like(l_a)
        if second is not None:
            total = jnp.sum(l_c[...], axis=1, keepdims=True)
            if not exact:
                big[...] = jnp.maximum(big[...], total)
            inv = 1.0 / total
            acc[...] = jnp.zeros_like(acc)

        def step(kb, masked):
            if second is not None:
                p = (p_c[kb] * inv).astype(jnp.bfloat16)
                acc[...] += jnp.dot(p, kv[kb, :, d:], preferred_element_type=jnp.float32)
            if first is not None:
                p = jnp.exp2((scores(first, kb, masked) - top) * scale)
                p_a[kb] = p
                l_a[...] += fold(p, jnp.add)

        @pl.loop(lo, hi)
        def _(kb):
            if first is None or exact:
                step(kb, exact)
            else:
                k_lo, k_hi = ends(kb)
                plain = (q_lo == q_hi) & (q_lo == k_lo) & (q_lo == k_hi)

                @pl.when(plain)
                def _():
                    step(kb, False)

                @pl.when(jnp.logical_not(plain))
                def _():
                    step(kb, True)

        if second is not None:
            out_ref[rows_of(second), cols_of(second)] = acc[...].astype(out_ref.dtype)

    big[...] = jnp.zeros_like(big)
    stage(0, None, 0)

    @pl.loop(0, (n - 1) // 2)
    def _(k):
        stage(2 * k + 1, 2 * k, 1)
        stage(2 * k + 2, 2 * k + 1, 2)

    for u in range(1 + 2 * ((n - 1) // 2), n):
        stage(u, u - 1, u)
    stage(None, n - 1, n)

    @pl.when(jnp.logical_not(jnp.max(big[...]) < 1e30))
    def _():
        @pl.loop(0, n)
        def _(u):
            stage(u, None, 0, True)
            stage(None, u, 1, True)


def attention(queries, kv_pieces, docs, q_doc, k_doc, start, rows):
    width = queries.shape[1]
    heads = width // HEAD_DIM
    bk = kv_pieces[0].shape[0]
    bq = min(Q_TILE, rows)
    here = start // rows
    grid_spec = pltpu.PrefetchScalarGridSpec(
        num_scalar_prefetch=1,
        grid=(1,),
        in_specs=[pl.BlockSpec((rows, width), lambda i, _: (here, 0))]
        + [pl.BlockSpec(memory_space=pl.ANY)] * 4
        + [pl.BlockSpec((rows, 1), lambda i, _: (here, 0)), pl.BlockSpec(k_doc.shape, lambda i, _: (0, 0, 0))],
        out_specs=pl.BlockSpec((rows, width), lambda i, _: (0, 0)),
        scratch_shapes=[pltpu.VMEM((4, bk, 2 * HEAD_DIM), jnp.bfloat16), pltpu.SemaphoreType.DMA((4,))]
        + [pltpu.VMEM((4, bq, bk), jnp.float32)] * 2
        + [pltpu.VMEM((bq, HEAD_DIM), jnp.float32)] * 3
        + [pltpu.VMEM((bq, 1), jnp.float32)],
    )
    return pl.pallas_call(
        functools.partial(attention_kernel, heads, bq, start),
        grid_spec=grid_spec,
        out_shape=jax.ShapeDtypeStruct((rows, width), jnp.bfloat16),
        compiler_params=pltpu.CompilerParams(vmem_limit_bytes=VMEM_LIMIT),
        cost_estimate=pl.CostEstimate(flops=16 * rows * 4 * bk * width, bytes_accessed=4 * rows * width, transcendentals=rows * 4 * bk * heads),
    )(docs, queries, *kv_pieces, q_doc, k_doc)


def solution(mesh):
    n_row = mesh.shape["row"]
    over_x = [(r, r ^ 2) for r in range(n_row)]
    over_core = [(r, r ^ 1) for r in range(n_row)]
    over_y = [(0, 1), (1, 0)]

    def far(piece):
        return lax.ppermute(piece, "row", over_x)

    def near(piece):
        return lax.ppermute(piece, "row", over_core)

    def after(value, *others):
        return lax.optimization_barrier((value,) + others)[0]

    def local_block(tokens, w_qkv, w_out, doc_ids):
        rows, cols = tokens.shape
        groups = (w_qkv.shape[1] - cols) // (2 * HEAD_DIM)
        q_cols = cols // groups
        g_cols = q_cols + 2 * HEAD_DIM
        out_at = [sum(OUT_CHUNKS[:c]) for c in range(len(OUT_CHUNKS))]
        out_ends = [lo + n for lo, n in zip(out_at, OUT_CHUNKS)]

        tokens_y = lax.ppermute(tokens, "col", over_y)
        docs_x = far(doc_ids)
        w_slice = w_qkv[:, :g_cols]
        w_far = [far(w_slice)]
        w_rest = after(w_qkv, w_slice)
        w_far += [far(w_rest[:, g * g_cols:(g + 1) * g_cols]) for g in range(1, groups)]
        w_near = near(w_qkv)
        docs = jnp.concatenate([doc_ids, near(doc_ids), docs_x, near(docs_x)])
        q_doc, k_doc = doc_ids.reshape(rows, 1), docs.reshape(n_row, 1, rows)
        wo_near = near(w_out)

        def project_group(g, x_y):
            w_last = near(w_far[g])
            q, kv = project([tokens], [x_y], w_qkv, w_near, w_far[g], w_last, g * g_cols, (q_cols, g_cols))
            kv_x = far(kv)
            return q, [kv, near(kv), kv_x, near(kv_x)]

        parts, spots = [], []

        def attend(g, q, pieces, start, size):
            context = attention(q, pieces, docs, q_doc, k_doc, start, size)
            context_y = lax.ppermute(context, "col", over_y)
            parts.extend([context, context_y])
            spots.extend([(True, g * q_cols, start), (False, g * q_cols, start)])
            return context

        q0, kv0 = project_group(0, tokens_y)
        q1, kv1 = project_group(1, after(tokens_y, kv0[0]))
        q2, kv2 = project_group(2, after(tokens_y, kv1[0]))
        out0 = attend(0, after(q0, q2), kv0, 0, rows)
        q3, kv3 = project_group(3, after(tokens_y, out0))
        out1 = attend(1, after(q1, q3), kv1, 0, rows)
        out2 = attend(2, after(q2, out1), kv2, 0, rows)
        out3 = attend(3, after(q3, out2), kv3, 0, rows // 2)
        attend(3, after(q3, out3), kv3, rows // 2, rows // 2)
        wo_rest = after(w_out, kv1[0])
        wo_far = [far(wo_rest[:, lo:hi]) for lo, hi in zip(out_at, out_ends)]
        result = None
        for c, first in enumerate(out_at):
            w_last = near(wo_far[c])
            result = combine(parts, spots, rows, w_out, wo_near, wo_far[c], w_last, first, result)
        return result

    row_spec = P(("data", "row"), "col")
    weight_spec = P("row", "col")
    return jax.shard_map(local_block, mesh=mesh, in_specs=(row_spec, weight_spec, weight_spec, P(("data", "row"))), out_specs=row_spec, check_vma=False)
```
